64 devices in a mesh: dp: 4 (over x, y), w: 16 (over z, core).
Axes of the slice: x: 2, y: 2, z: 8, core: 2. Of those that a mesh axis runs over, the one named last changes fastest.
The devices are a block of a 4x4x8 slice.
Arguments:
- hidden: bfloat16 [1024, 64, 1152], P(('dp', 'w')), parts along dimension 0
- lengths: int32 [1024], P(('dp', 'w')), parts along dimension 0
- attn_norm: bfloat16 [2, 1152], P(None, 'w')
- w_q: bfloat16 [2, 1152, 1024], P(None, 'w')
- w_k: bfloat16 [2, 1152, 256], P(None, 'w')
- w_v: bfloat16 [2, 1152, 256], P(None, 'w')
- w_o: bfloat16 [2, 1024, 1152], P(None, 'w')
- mlp_norm: bfloat16 [2, 1152], P(None, 'w')
- w_gate: bfloat16 [2, 1152, 6912], P(None, 'w')
- w_up: bfloat16 [2, 1152, 6912], P(None, 'w')
- w_down: bfloat16 [2, 6912, 1152], P(None, 'w')
Outputs:
- output 1: bfloat16 [1024, 64, 1152], P(('dp', 'w')), parts along dimension 0
- output 2: bfloat16 [2, 1024, 64, 1, 256], P(None, ('dp', 'w')), parts along dimension 1
- output 3: bfloat16 [2, 1024, 64, 1, 256], P(None, ('dp', 'w')), parts along dimension 1
There are 4 independent parts. The reference program is written for one: setup_inputs(seed, part) draws one part's arguments, and reference() takes and returns one part's arrays. A program takes and returns all parts, laid end to end along the dimension named above; an argument that names none is the same for every part.
All inputs are finite; a program needn't handle non-finite values.
Results may differ from the reference program's by a relative error of at most 0.0130315.
Values are sent between devices in bfloat16 or wider.
A program may use at most 768 MiB of HBM per device.

```python
import jax
import jax.numpy as jnp
from jax import lax

D_MODEL = 1152
N_HEADS = 4
KV_HEADS = 1
HEAD_DIM = 256
D_FF = 6912
SEQ_LEN = 64
N_SEQS = 256
N_LAYERS = 2
RMS_EPS = 1e-6
ROPE_THETA = 10000.0
QUERY_BLOCK = min(SEQ_LEN, 512)
GROUP_SIZE = N_HEADS // KV_HEADS


def weight_draw(key_w, weight_shape, weight_scale):
    return (jax.random.normal(key_w, weight_shape, jnp.float32) * weight_scale).astype(jnp.bfloat16)


def setup_inputs(seed: int = 0, part: int = 0) -> dict:
    part_key = jax.random.fold_in(jax.random.key(seed), part)
    key_hidden, key_len, key_full = jax.random.split(part_key, 3)
    hidden = jax.random.normal(key_hidden, (N_SEQS, SEQ_LEN, D_MODEL), jnp.float32).astype(jnp.bfloat16)
    drawn_len = jax.random.randint(key_len, (N_SEQS,), max(1, SEQ_LEN // 8), SEQ_LEN + 1)
    full_idx = jax.random.randint(key_full, (), 0, N_SEQS)
    lengths = jnp.where(jnp.arange(N_SEQS) == full_idx, SEQ_LEN, drawn_len).astype(jnp.int32)
    weight_keys = jax.random.split(jax.random.key(seed + 1), 9)
    q_width = N_HEADS * HEAD_DIM
    kv_width = KV_HEADS * HEAD_DIM
    d_scale = D_MODEL ** -0.5
    return {
        'hidden': hidden,
        'lengths': lengths,
        'attn_norm': weight_draw(weight_keys[0], (N_LAYERS, D_MODEL), 0.5),
        'w_q': weight_draw(weight_keys[1], (N_LAYERS, D_MODEL, q_width), 1.5 * d_scale),
        'w_k': weight_draw(weight_keys[2], (N_LAYERS, D_MODEL, kv_width), 1.5 * d_scale),
        'w_v': weight_draw(weight_keys[3], (N_LAYERS, D_MODEL, kv_width), d_scale),
        'w_o': weight_draw(weight_keys[4], (N_LAYERS, q_width, D_MODEL), q_width ** -0.5),
        'mlp_norm': weight_draw(weight_keys[5], (N_LAYERS, D_MODEL), 0.5),
        'w_gate': weight_draw(weight_keys[6], (N_LAYERS, D_MODEL, D_FF), d_scale),
        'w_up': weight_draw(weight_keys[7], (N_LAYERS, D_MODEL, D_FF), d_scale),
        'w_down': weight_draw(weight_keys[8], (N_LAYERS, D_FF, D_MODEL), D_FF ** -0.5),
    }


def rms_norm(hidden_f, norm_gain):
    mean_sq = jnp.mean(hidden_f * hidden_f, axis=-1, keepdims=True)
    return (hidden_f * lax.rsqrt(mean_sq + RMS_EPS) * (1.0 + norm_gain.astype(jnp.float32))).astype(jnp.bfloat16)


def rope_tables():
    half_dim = HEAD_DIM // 2
    inv_freq = ROPE_THETA ** (-2.0 * jnp.arange(half_dim, dtype=jnp.float32) / HEAD_DIM)
    angles = jnp.arange(SEQ_LEN, dtype=jnp.float32)[:, None] * inv_freq[None, :]
    return jnp.cos(angles)[:, None, :], jnp.sin(angles)[:, None, :]


def apply_rope(projected, cos_tab, sin_tab):
    half_dim = HEAD_DIM // 2
    first_half = projected[..., :half_dim]
    second_half = projected[..., half_dim:]
    return jnp.concatenate([first_half * cos_tab - second_half * sin_tab, second_half * cos_tab + first_half * sin_tab], axis=-1)


def seq_attention(q_rope, k_rope, v_proj, length):
    key_pos = jnp.arange(SEQ_LEN)
    keys_f = k_rope.astype(jnp.float32)
    values_f = v_proj.astype(jnp.float32)

    def one_block(block_idx):
        q_start = block_idx * QUERY_BLOCK
        q_blk = lax.dynamic_slice_in_dim(q_rope, q_start, QUERY_BLOCK, 0).astype(jnp.float32)
        q_pos = q_start + jnp.arange(QUERY_BLOCK)
        scores = jnp.einsum('qhgd,shd->hgqs', q_blk, keys_f)
        allowed = (key_pos[None, :] <= q_pos[:, None]) & (key_pos[None, :] < length)
        scores = jnp.where(allowed, scores, -1e30)
        scores = scores - jnp.max(scores, axis=-1, keepdims=True)
        exp_scores = jnp.exp(scores)
        attn_probs = exp_scores / jnp.sum(exp_scores, axis=-1, keepdims=True)
        attn_probs = jnp.where((q_pos < length)[:, None], attn_probs, 0.0).astype(jnp.bfloat16)
        return jnp.einsum('hgqs,shd->qhgd', attn_probs.astype(jnp.float32), values_f).astype(jnp.bfloat16)

    blocks = lax.map(one_block, jnp.arange(SEQ_LEN // QUERY_BLOCK))
    return blocks.reshape(SEQ_LEN, N_HEADS * HEAD_DIM)


def one_layer(hidden, length, params):
    attn_gain, wq_layer, wk_layer, wv_layer, wo_layer, mlp_gain, wg_layer, wu_layer, wd_layer = params
    cos_tab, sin_tab = rope_tables()
    hidden_f = hidden.astype(jnp.float32)
    normed = rms_norm(hidden_f, attn_gain)
    q_proj = jnp.dot(normed, wq_layer, preferred_element_type=jnp.float32).reshape(SEQ_LEN, N_HEADS, HEAD_DIM)
    k_proj = jnp.dot(normed, wk_layer, preferred_element_type=jnp.float32).reshape(SEQ_LEN, KV_HEADS, HEAD_DIM)
    v_proj = jnp.dot(normed, wv_layer, preferred_element_type=jnp.float32).astype(jnp.bfloat16).reshape(SEQ_LEN, KV_HEADS, HEAD_DIM)
    q_rope = (apply_rope(q_proj, cos_tab, sin_tab) * HEAD_DIM ** -0.5).astype(jnp.bfloat16).reshape(SEQ_LEN, KV_HEADS, GROUP_SIZE, HEAD_DIM)
    k_rope = apply_rope(k_proj, cos_tab, sin_tab).astype(jnp.bfloat16)
    attn_out = seq_attention(q_rope, k_rope, v_proj, length)
    mixed_bf = (hidden_f + jnp.dot(attn_out, wo_layer, preferred_element_type=jnp.float32)).astype(jnp.bfloat16)
    mixed_f = mixed_bf.astype(jnp.float32)
    normed_mlp = rms_norm(mixed_f, mlp_gain)
    gate_proj = jnp.dot(normed_mlp, wg_layer, preferred_element_type=jnp.float32)
    up_proj = jnp.dot(normed_mlp, wu_layer, preferred_element_type=jnp.float32)
    act_bf = (jax.nn.gelu(gate_proj, approximate=True) * up_proj).astype(jnp.bfloat16)
    new_hidden = (mixed_f + jnp.dot(act_bf, wd_layer, preferred_element_type=jnp.float32)).astype(jnp.bfloat16)
    return new_hidden, k_rope, v_proj


def reference(hidden, lengths, attn_norm, w_q, w_k, w_v, w_o, mlp_norm, w_gate, w_up, w_down):
    stacked = (attn_norm, w_q, w_k, w_v, w_o, mlp_norm, w_gate, w_up, w_down)

    def one_seq(seq_args):
        seq_hidden, length = seq_args

        def layer_step(carry_hidden, params):
            new_hidden, k_rope, v_proj = one_layer(carry_hidden, length, params)
            return new_hidden, (k_rope, v_proj)

        final_hidden, kv_pair = lax.scan(layer_step, seq_hidden, stacked)
        return final_hidden, kv_pair[0], kv_pair[1]

    out_hidden, k_all, v_all = lax.map(one_seq, (hidden, lengths))
    return out_hidden, jnp.transpose(k_all, (1, 0, 2, 3, 4)), jnp.transpose(v_all, (1, 0, 2, 3, 4))
```

```python
import functools
import math

import jax
import jax.numpy as jnp
import numpy as np
from jax import lax
from jax.experimental import pallas as pl
from jax.experimental.pallas import tpu as pltpu
from jax.sharding import PartitionSpec as P

HEAD_DIM = 256
HALF = HEAD_DIM // 2
RMS_EPS = 1e-6
ROPE_THETA = 10000.0
MESH = pl.DeviceIdType.MESH
ROWS = 256
COL = 768
DCOL = 384
LAG = 2


def rms(x, gain):
    mean_sq = jnp.mean(x * x, axis=-1, keepdims=True)
    return (x * lax.rsqrt(mean_sq + RMS_EPS) * (1.0 + gain)).astype(jnp.bfloat16)


class Plan:
    def __init__(self, mesh, hidden, wq, wk, wv, wo, wg, wd):
        self.nw = mesh.shape["w"]
        self.nz = self.nw // 2
        self.side = math.isqrt(mesh.shape["dp"])
        self.layers = wq.shape[0]
        self.prompts, self.seq, self.width = hidden.shape
        self.tokens = self.prompts * self.seq
        self.kr = wq.shape[1]
        self.qw, self.kw = wq.shape[2], wk.shape[2]
        self.acols = self.qw + 2 * self.kw
        self.orow = wo.shape[1]
        self.ff = wg.shape[2]
        self.drow = wd.shape[1]
        self.na = self.ff // COL + 1
        self.nd = self.width // DCOL
        self.per_layer = self.na + 1 + self.nd
        self.steps = self.layers * self.per_layer
        self.heads = self.qw // HEAD_DIM


def body(pn, compute, len_ref, cos_ref, sin_ref, ag_ref, mg_ref, h_in, wq, wk, wv, wo, wg, wu, wd,
         out_h, out_k, out_v, la, lo, ld,
         h, r, q, kk, vv, o, a, wa, wob, wdb,
         own_sem, zs, zr, ps, pr, load_sem, io_sem):
    w = lax.axis_index("w")
    dp = lax.axis_index("dp")
    z, c = w // 2, w % 2
    nz = pn.nz
    gx, gy = dp // pn.side, dp % pn.side
    par = (gx + gy) % 2
    s = 1 - 2 * c
    up_w = lax.rem(z + 1, nz) * 2 + c
    dn_w = lax.rem(z + nz - 1, nz) * 2 + c
    far_w = lax.rem(z + s + nz, nz) * 2 + c
    mate_w = z * 2 + 1 - c
    x_dp = (gx + 1 - 2 * (gx % 2)) * pn.side + gy
    y_dp = gx * pn.side + gy + 1 - 2 * (gy % 2)
    dev_up, dev_dn, dev_far = (dp, up_w), (dp, dn_w), (dp, far_w)
    dev_mate, dev_x, dev_y = (dp, mate_w), (x_dp, w), (y_dp, w)
    farslot = nz // 2
    outs_up = [(0, 1), (1, 2), (2, 3)]
    outs_dn = [(0, 7), (7, 6), (6, 5)]

    barrier = pltpu.get_barrier_semaphore()
    for dev in (dev_up, dev_dn, dev_mate, dev_x, dev_y):
        pl.semaphore_signal(barrier, inc=1, device_id=dev, device_id_type=MESH)
    pl.semaphore_wait(barrier, 5)

    def split(g):
        return g // pn.per_layer, g % pn.per_layer

    def view_a(l, k, e, core, piece, half):
        off, size = {"all": (0, pn.acols), "half": (half * COL, COL), "x": (half * COL, COL // 2),
                     "y": (half * COL + COL // 2, COL // 2)}[piece]
        cols = slice(None) if piece == "all" else pl.ds(pl.multiple_of(off, 128), size)
        return la.at[l, k, e, pl.ds(pl.multiple_of(core * pn.kr, 8), pn.kr), cols]

    def view_o(l, k, e, core, piece, half):
        hr = pn.orow // 2
        off, size = {"all": (0, pn.orow), "half": (half * hr, hr), "x": (half * hr, hr // 2),
                     "y": (half * hr + hr // 2, hr // 2)}[piece]
        return lo.at[l, e, pl.ds(pl.multiple_of(core * pn.orow + off, 16), size), :]

    def view_d(l, k, e, core, piece, half):
        hr = pn.drow // 2
        hx = -(-hr // 16) * 8
        off, size = {"all": (0, pn.drow), "half": (half * hr, hr), "x": (half * hr, hx),
                     "y": (half * hr + hx, hr - hx)}[piece]
        return ld.at[l, k, e, pl.ds(pl.multiple_of(core * pn.drow + off, 8), size), :]

    def by_type(g, fn):
        l, i = split(g)

        @pl.when((i == 0) | ((i >= 2) & (i <= pn.na)))
        def _():
            fn(functools.partial(view_a, l, jnp.where(i == 0, 0, i - 1)))

        @pl.when(i == 1)
        def _():
            fn(functools.partial(view_o, l, 0))

        @pl.when(i > pn.na)
        def _():
            fn(functools.partial(view_d, l, i - pn.na - 1))

    def copy(src, dst, ss, rs, dev):
        return pltpu.make_async_remote_copy(src_ref=src, dst_ref=dst, send_sem=ss, recv_sem=rs,
                                            device_id=dev, device_id_type=MESH)

    def zsend(g, view, j, src, dst, dev):
        return copy(view(src, c, "half", par), view(dst, c, "half", par), zs.at[g, j], zr.at[g, j], dev)

    def arrived(g, view, j, slot):
        v = view(slot, c, "half", par)
        copy(v, v, zs.at[g, j], zr.at[g, j], dev_up).wait_recv()

    rest = pl.ds(1, nz - 1)

    def own_copies(l, i):
        me = pl.ds(pl.multiple_of(c * pn.kr, 8), pn.kr)
        if i == 0:
            return [(wq.at[l], la.at[l, 0, 0, me, pl.ds(0, pn.qw)]),
                    (wk.at[l], la.at[l, 0, 0, me, pl.ds(pn.qw, pn.kw)]),
                    (wv.at[l], la.at[l, 0, 0, me, pl.ds(pn.qw + pn.kw, pn.kw)])]
        if i == 1:
            return [(wo.at[l], view_o(l, 0, 0, c, "all", 0))]
        if i <= pn.na:
            k = i - 1
            return [(wg.at[l, :, pl.ds((k - 1) * COL, COL)], la.at[l, k, 0, me, pl.ds(0, COL)]),
                    (wu.at[l, :, pl.ds((k - 1) * COL, COL)], la.at[l, k, 0, me, pl.ds(COL, COL)])]
        k = i - pn.na - 1
        return [(wd.at[l, :, pl.ds(k * DCOL, DCOL)], view_d(l, k, 0, c, "all", 0))]

    for l in range(pn.layers):
        for i in range(pn.per_layer):
            for j, (src, dst) in enumerate(own_copies(l, i)):
                pltpu.make_async_copy(src, dst, own_sem.at[l * pn.per_layer + i]).start()

    def stage0(g):
        def fn(view):
            v = view(0, c, "all", 0)
            pltpu.make_async_copy(v, v, own_sem.at[g]).wait()
            zsend(g, view, 0, 0, 1, dev_up).start()
            zsend(g, view, 1, 0, nz - 1, dev_dn).start()
        by_type(g, fn)

    def stage_hop(n, g):
        def fn(view):
            arrived(g, view, 2 * n - 2, n)
            zsend(g, view, 2 * n, n, n + 1, dev_up).start()
            arrived(g, view, 2 * n - 1, nz - n)
            zsend(g, view, 2 * n + 1, nz - n, nz - n - 1, dev_dn).start()
            for j in (2 * n - 2, 2 * n - 1):
                zsend(g, view, j, 0, 1, dev_up).wait_send()
        by_type(g, fn)

    def stage3(g):
        def fn(view):
            arrived(g, view, 4, 3)
            arrived(g, view, 5, nz - 3)
            zsend(g, view, 6, farslot - s, farslot, dev_far).start()
            for j in (4, 5):
                zsend(g, view, j, 0, 1, dev_up).wait_send()
        by_type(g, fn)

    def xy(g, view, which, half, dev):
        v = view(rest, c, which, half)
        j = 0 if which == "x" else 1
        return copy(v, v, ps.at[g, j], pr.at[g, j], dev)

    def stage4(g):
        def fn(view):
            arrived(g, view, 6, farslot)
            xy(g, view, "x", par, dev_x).start()
            xy(g, view, "y", par, dev_y).start()
            zsend(g, view, 6, 0, 1, dev_up).wait_send()
        by_type(g, fn)

    def mate(g, view, core):
        v = view(slice(None), core, "all", 0)
        return copy(v, v, ps.at[g, 2], pr.at[g, 2], dev_mate)

    def stage5(g):
        def fn(view):
            xy(g, view, "x", 1 - par, dev_x).wait_recv()
            xy(g, view, "y", 1 - par, dev_y).wait_recv()
            mate(g, view, c).start()
            xy(g, view, "x", par, dev_x).wait_send()
            xy(g, view, "y", par, dev_y).wait_send()
        by_type(g, fn)

    def load_one(l, i, e):
        zz = lax.rem(z + nz - e, nz)

        def rows(n):
            return pl.ds(pl.multiple_of(zz * 2 * n, 16), 2 * n)
        return zz, rows

    def loads(g, go):
        l, i = split(g)

        @pl.when((i == 0) | ((i >= 2) & (i <= pn.na)))
        def _():
            k = jnp.where(i == 0, 0, i - 1)
            b = lax.rem(l * pn.na + k, 3)
            if go:
                for e in range(nz):
                    _, rows = load_one(l, i, e)
                    pltpu.make_async_copy(la.at[l, k, e], wa.at[b, rows(pn.kr), :], load_sem.at[b]).start()
            else:
                pltpu.make_async_copy(wa.at[b], wa.at[b], load_sem.at[b]).wait()

        @pl.when(i == 1)
        def _():
            if go:
                for e in range(nz):
                    _, rows = load_one(l, i, e)
                    pltpu.make_async_copy(lo.at[l, e], wob.at[rows(pn.orow), :], load_sem.at[3]).start()
            else:
                pltpu.make_async_copy(wob, wob, load_sem.at[3]).wait()

        @pl.when(i > pn.na)
        def _():
            k = i - pn.na - 1
            b = lax.rem(l * pn.nd + k, 2)
            if go:
                for e in range(nz):
                    _, rows = load_one(l, i, e)
                    pltpu.make_async_copy(ld.at[l, k, e], wdb.at[b, rows(pn.drow), :], load_sem.at[4 + b]).start()
            else:
                pltpu.make_async_copy(wdb.at[b], wdb.at[b], load_sem.at[4 + b]).wait()

    def stage6(g):
        def fn(view):
            mate(g, view, 1 - c).wait_recv()
            mate(g, view, c).wait_send()
        by_type(g, fn)
        loads(g, True)

    tiles = pn.tokens // ROWS

    def tile(t):
        return pl.ds(pl.multiple_of(t * ROWS, ROWS), ROWS)

    def unit_qkv(l):
        b = lax.rem(l * pn.na, 3)
        gain = ag_ref[l]

        def step(t, _):
            rr = tile(t)
            normed = rms(h[rr, :].astype(jnp.float32), gain)
            cos, sin = cos_ref[...], sin_ref[...]

            def rope(p):
                first, second = p[:, :HALF], p[:, HALF:]
                return first * cos - second * sin, second * cos + first * sin
            for hh in range(pn.heads):
                cols = pl.ds(hh * HEAD_DIM, HEAD_DIM)
                first, second = rope(jnp.dot(normed, wa[b, :, cols], preferred_element_type=jnp.float32))
                q[rr, pl.ds(hh * HEAD_DIM, HALF)] = (first * HEAD_DIM ** -0.5).astype(jnp.bfloat16)
                q[rr, pl.ds(hh * HEAD_DIM + HALF, HALF)] = (second * HEAD_DIM ** -0.5).astype(jnp.bfloat16)
            first, second = rope(jnp.dot(normed, wa[b, :, pl.ds(pn.qw, pn.kw)], preferred_element_type=jnp.float32))
            kk[l, rr, pl.ds(0, HALF)] = first.astype(jnp.bfloat16)
            kk[l, rr, pl.ds(HALF, HALF)] = second.astype(jnp.bfloat16)
            vv[l, rr, :] = jnp.dot(normed, wa[b, :, pl.ds(pn.qw + pn.kw, pn.kw)],
                                   preferred_element_type=jnp.float32).astype(jnp.bfloat16)
            return 0
        lax.fori_loop(0, tiles, step, 0)
        for j, (src, dst) in enumerate(((kk, out_k), (vv, out_v))):
            pltpu.make_async_copy(src.at[l], dst.at[l], io_sem.at[1 + 2 * l + j]).start()

    def unit_attn(l, lo_pair, hi_pair):
        two = 2 * pn.seq
        shape = (pn.heads * two, two)
        row = lax.broadcasted_iota(jnp.int32, shape, 0) % two
        col = lax.broadcasted_iota(jnp.int32, shape, 1)
        rp, cp = row // pn.seq, col // pn.seq
        qpos, kpos = row % pn.seq, col % pn.seq
        causal = (rp == cp) & (kpos <= qpos)

        def step(t, _):
            rr = pl.ds(pl.multiple_of(t * two, two), two)
            len0, len1 = len_ref[2 * t], len_ref[2 * t + 1]
            qs = q[rr, :]
            stacked = jnp.concatenate([qs[:, i * HEAD_DIM:(i + 1) * HEAD_DIM] for i in range(pn.heads)], axis=0)
            sc = lax.dot_general(stacked, kk[l, rr, :], (((1,), (1,)), ((), ())), preferred_element_type=jnp.float32)
            allowed = causal & (kpos < jnp.where(cp == 0, len0, len1))
            sc = jnp.where(allowed, sc, -1e30)
            sc = jnp.exp(sc - jnp.max(sc, axis=-1, keepdims=True))
            pr_ = sc / jnp.sum(sc, axis=-1, keepdims=True)
            live = qpos < jnp.where(rp == 0, len0, len1)
            pr_ = jnp.where(live, pr_, 0.0).astype(jnp.bfloat16)
            ov = jnp.dot(pr_, vv[l, rr, :], preferred_element_type=jnp.float32).astype(jnp.bfloat16)
            for i in range(pn.heads):
                o[rr, pl.ds(i * HEAD_DIM, HEAD_DIM)] = ov[i * two:(i + 1) * two, :]
            return 0
        lax.fori_loop(lo_pair, hi_pair, step, 0)

    def unit_o(l):
        gain = mg_ref[l]

        def step(t, _):
            rr = tile(t)
            mixed = h[rr, :].astype(jnp.float32) + jnp.dot(o[rr, :], wob[...], preferred_element_type=jnp.float32)
            mixed = mixed.astype(jnp.bfloat16)
            h[rr, :] = mixed
            r[rr, :] = rms(mixed.astype(jnp.float32), gain)
            return 0
        lax.fori_loop(0, tiles, step, 0)

    def unit_mlp(l, k):
        b = lax.rem(l * pn.na + k, 3)

        def step(t, _):
            rr = tile(t)
            x = r[rr, :]
            for j in range(COL // 256):
                gp = jnp.dot(x, wa[b, :, pl.ds(j * 256, 256)], preferred_element_type=jnp.float32)
                upv = jnp.dot(x, wa[b, :, pl.ds(COL + j * 256, 256)], preferred_element_type=jnp.float32)
                act = (jax.nn.gelu(gp, approximate=True) * upv).astype(jnp.bfloat16)
                a[rr, pl.ds(pl.multiple_of((k - 1) * COL + j * 256, 256), 256)] = act
            return 0
        lax.fori_loop(0, tiles, step, 0)

    def unit_down(l, k):
        b = lax.rem(l * pn.nd + k, 2)
        cols = pl.ds(pl.multiple_of(k * DCOL, 128), DCOL)

        def step(t, _):
            rr = tile(t)
            acc = jnp.dot(a[rr, :], wdb[b], preferred_element_type=jnp.float32)
            h[rr, cols] = (h[rr, cols].astype(jnp.float32) + acc).astype(jnp.bfloat16)
            return 0
        lax.fori_loop(0, tiles, step, 0)

    pairs = pn.prompts // 2
    pltpu.make_async_copy(h_in, h, io_sem.at[0]).start()
    pltpu.make_async_copy(h_in, h, io_sem.at[0]).wait()

    last = 6 * LAG

    def run_units(t):
        g = t - last - 1
        l, i = split(g)
        g2 = g - 1
        l2, i2 = split(g2)

        @pl.when((g >= 0) & (g < pn.steps))
        def _():
            loads(g, False)

        if not compute:
            return

        @pl.when((g2 >= 0) & (i2 >= 2) & (i2 <= pn.na))
        def _():
            unit_mlp(l2, i2 - 1)

        @pl.when((g >= 0) & (g < pn.steps))
        def _():
            @pl.when(i == 0)
            def _():
                unit_qkv(l)

            @pl.when(i == 1)
            def _():
                unit_attn(l, 0, pairs // 2)

            @pl.when(i == 2)
            def _():
                unit_attn(l, pairs // 2, pairs)
                unit_o(l)

            @pl.when(i > pn.na)
            def _():
                unit_down(l, i - pn.na - 1)

    stages = [stage0, functools.partial(stage_hop, 1), functools.partial(stage_hop, 2), stage3, stage4, stage5, stage6]

    def tick(t, _):
        for n in range(len(stages) - 1, -1, -1):
            g = t - n * LAG

            @pl.when((g >= 0) & (g < pn.steps))
            def _(n=n, g=g):
                stages[n](g)
        run_units(t)
        return 0
    lax.fori_loop(0, pn.steps + last + 1, tick, 0)

    out = pltpu.make_async_copy(h, out_h, io_sem.at[0])
    out.start()
    if compute:
        for l in range(pn.layers):
            for j, (src, dst) in enumerate(((kk, out_k), (vv, out_v))):
                pltpu.make_async_copy(src.at[l], dst.at[l], io_sem.at[1 + 2 * l + j]).wait()
    out.wait()


def make(mesh, compute=True):
    batch_spec = P(('dp', 'w'))
    weight_spec = P(None, 'w')
    cache_spec = P(None, ('dp', 'w'))

    def device_fn(hidden, lengths, attn_norm, w_q, w_k, w_v, w_o, mlp_norm, w_gate, w_up, w_down):
        pn = Plan(mesh, hidden, w_q, w_k, w_v, w_o, w_gate, w_down)
        norms = lax.all_gather(jnp.stack([attn_norm, mlp_norm]), 'w', axis=2, tiled=True)
        norms = norms.astype(jnp.float32)[:, :, None, :]
        inv_freq = np.float32(ROPE_THETA) ** (np.float32(-2.0) * np.arange(HALF, dtype=np.float32) / np.float32(HEAD_DIM))
        angles = np.arange(pn.seq, dtype=np.float32)[:, None] * inv_freq[None, :].astype(np.float32)
        reps = ROWS // pn.seq
        cos = jnp.asarray(np.tile(np.cos(angles).astype(np.float32), (reps, 1)))
        sin = jnp.asarray(np.tile(np.sin(angles).astype(np.float32), (reps, 1)))
        bf = jnp.bfloat16
        nz, S = pn.nz, jax.ShapeDtypeStruct
        L, T = pn.layers, pn.tokens
        vm = pl.BlockSpec(memory_space=pltpu.VMEM)
        anyspec = pl.BlockSpec(memory_space=pl.ANY)
        outs = pl.pallas_call(
            functools.partial(body, pn, compute),
            name="layers",
            out_shape=(S((T, pn.width), bf), S((L, T, pn.kw), bf), S((L, T, pn.kw), bf),
                       S((L, pn.na, nz, 2 * pn.kr, pn.acols), bf),
                       S((L, nz, 2 * pn.orow, pn.width), bf),
                       S((L, pn.nd, nz, 2 * pn.drow, DCOL), bf)),
            in_specs=[pl.BlockSpec(memory_space=pltpu.SMEM), vm, vm, vm, vm] + [anyspec] * 8,
            out_specs=(anyspec,) * 6,
            scratch_shapes=[
                pltpu.VMEM((T, pn.width), bf), pltpu.VMEM((T, pn.width), bf),
                pltpu.VMEM((T, pn.qw), bf), pltpu.VMEM((L, T, pn.kw), bf), pltpu.VMEM((L, T, pn.kw), bf),
                pltpu.VMEM((T, pn.qw), bf), pltpu.VMEM((T, pn.ff), bf),
                pltpu.VMEM((3, pn.width, pn.acols), bf), pltpu.VMEM((pn.qw, pn.width), bf),
                pltpu.VMEM((2, pn.ff, DCOL), bf),
                pltpu.SemaphoreType.DMA((pn.steps,)),
                pltpu.SemaphoreType.DMA((pn.steps, nz - 1)), pltpu.SemaphoreType.DMA((pn.steps, nz - 1)),
                pltpu.SemaphoreType.DMA((pn.steps, 3)), pltpu.SemaphoreType.DMA((pn.steps, 3)),
                pltpu.SemaphoreType.DMA((6,)), pltpu.SemaphoreType.DMA((1 + 2 * L,)),
            ],
            compiler_params=pltpu.CompilerParams(collective_id=0, has_side_effects=True, vmem_limit_bytes=63 << 20),
        )(lengths, cos, sin, norms[0], norms[1], hidden.reshape(T, pn.width), w_q, w_k, w_v, w_o, w_gate, w_up, w_down)
        cache = (L, pn.prompts, pn.seq, pn.kw // HEAD_DIM, HEAD_DIM)
        return outs[0].reshape(hidden.shape), outs[1].reshape(cache), outs[2].reshape(cache)

    return jax.shard_map(device_fn, mesh=mesh, in_specs=(batch_spec, batch_spec) + (weight_spec,) * 9,
                         out_specs=(batch_spec, cache_spec, cache_spec), check_vma=False)


def solution(mesh):
    return make(mesh)
```
